32 devices in a mesh: group: 2 (over y), hi: 4 (over z), lo: 2 (over x), cuts: 2 (over core).
Axes of the slice: x: 2, y: 2, z: 4, core: 2. Of those that a mesh axis runs over, the one named last changes fastest.
Arguments:
- state_block: float32 [8, 2, 131072], P(('group', 'hi'), 'lo'), parts along dimension 0, may hold values from -6 to 6
- gate_table: float32 [4, 256, 256], replicated, may hold values from -0.375 to 0.375
- closing_table: float32 [4, 2, 2, 256], replicated, may hold values from -1 to 1
- slice_edges: int32 [8, 3], P(('group', 'cuts')), parts along dimension 0, may hold values from 0 to 3
- bit_orders: int32 [2, 8], replicated, may hold values from 0 to 7, each once within a row
Outputs:
- amplitudes: float32 [8, 2, 65536], P(('group', 'hi'), 'lo', 'cuts'), parts along dimension 0
The draws below stay inside these ranges and needn't reach their ends.
There are 2 independent parts, one for each index of `group`. The reference program is written for one: setup_inputs(seed, part) draws one part's arguments, and reference() takes and returns one part's arrays. A program takes and returns all parts, laid end to end along the dimension named above; an argument that names none is the same for every part. Nothing has to cross between parts.
Inputs may be any that keep to these rules, and one draw needn't show every extreme that they name: `bit_orders`: each row is a permutation of 0 to 7.
All inputs are finite; a program needn't handle non-finite values.
Results may differ from the reference program's by a relative error of at most 0.0001.
Values sent between devices are 32-bit elements; how exact they have to be, the bound alone decides.
A program may use at most 64 MiB of HBM per device.

```python
import jax
import jax.numpy as jnp
from jax import lax

BITS = 8
GATE = 256
CLOSED = 2
MIDDLE = 1
EDGES = 4
SLICES = 4
HI_SPAN = 64
LO_SPAN = 128
LOCAL = 131072
AMPS = 65536
N_HI = 4
N_LO = 2


def plant(entries, key, least, high):
    shape = entries.shape
    spot = [jax.random.randint(jax.random.fold_in(key, axis), (), 0, shape[axis]) for axis in range(len(shape))]
    entries = entries.at[tuple(spot)].set(least)
    longest = shape.index(max(shape))
    spot[longest] = (spot[longest] + 1) % shape[longest]
    return entries.at[tuple(spot)].set(high)


def block_levels(stream_key, extent, cuts, low, high):
    loudness = 1.0
    for position, parts in cuts:
        heights = jax.random.uniform(jax.random.fold_in(jax.random.fold_in(stream_key, 6), position), (parts,), jnp.float32, low / len(cuts), high / len(cuts))
        loudness = loudness * jnp.repeat(jnp.exp(heights), extent[position] // parts).reshape((-1,) + (1,) * (len(extent) - 1 - position))
    return loudness


def gaussian(own_key, extent, scale, limit, cuts=(), kind=jnp.bfloat16):
    drawn = scale * jax.random.normal(own_key, extent, jnp.float32)
    if cuts:
        drawn = drawn * block_levels(own_key, extent, cuts, -0.22, 0.18)
    return jnp.clip(drawn, -limit, limit).astype(kind)


def setup_inputs(seed: int = 0, part: int = 0) -> dict:
    splits = jax.random.split(jax.random.key(seed), 6)
    own_keys = jax.random.split(jax.random.fold_in(splits[5], part), 6)
    return {
        "state_block": gaussian(own_keys[0], (N_HI, N_LO, LOCAL), 1.0, 6.0, ((0, 4), (1, 2)), jnp.float32),
        "gate_table": gaussian(splits[1], (EDGES, GATE, GATE), GATE ** -0.5, 0.375, (), jnp.float32),
        "closing_table": jnp.clip(jax.random.uniform(splits[2], (EDGES, 2, CLOSED, GATE), jnp.float32, -1.0, 1.0), -1.0, 1.0),
        "slice_edges": plant(jax.random.randint(own_keys[3], (SLICES, 3), 0, EDGES), jax.random.fold_in(own_keys[3], 1), 0, EDGES - 1).astype(jnp.int32),
        "bit_orders": jax.vmap(lambda own: jax.random.permutation(own, BITS))(jax.random.split(splits[4], 2)).reshape((2, BITS)).astype(jnp.int32),
    }


def permuted(gate, order):
    rows = jnp.arange(GATE, dtype=jnp.int32)
    picked = (rows[:, None] >> order[None, :].astype(jnp.int32)) & 1
    weights = jnp.left_shift(jnp.ones((BITS,), jnp.int32), jnp.arange(BITS, dtype=jnp.int32))
    source = jnp.sum(picked * weights[None, :], axis=1).astype(jnp.int32)
    return jnp.take(gate, source, axis=0)


def reference(state_block, gate_table, closing_table, slice_edges, bit_orders):
    tensor = state_block.reshape(N_HI, N_LO, HI_SPAN, N_HI, CLOSED, MIDDLE, N_LO, LO_SPAN)
    total = jnp.zeros((N_HI, N_LO, AMPS), jnp.float32)
    for slice_index in range(SLICES):
        chosen = slice_edges[slice_index]
        first = permuted(gate_table[chosen[0]], bit_orders[0]).reshape(HI_SPAN, N_HI, HI_SPAN, N_HI)
        second = permuted(gate_table[chosen[1]], bit_orders[1]).reshape(N_LO, LO_SPAN, N_LO, LO_SPAN)
        front = closing_table[chosen[2], 0].reshape(CLOSED, HI_SPAN, N_HI)
        rear = closing_table[chosen[2], 1].reshape(CLOSED, N_LO, LO_SPAN)
        section_one = jnp.einsum('phPH,hlpbzmeq->HlPbzmeq', first, tensor, precision=lax.Precision.HIGHEST)
        weight_one = jnp.transpose(front, (2, 1, 0))
        section_one = section_one * weight_one[:, None, :, None, :, None, None, None]
        section_two = jnp.einsum('lqLQ,hlpbzmeq->hLpbzmeQ', second, section_one, precision=lax.Precision.HIGHEST)
        closed = jnp.einsum('zLQ,hLpbzmeQ->hLpbmeQ', rear, section_two, precision=lax.Precision.HIGHEST)
        total = total + closed.reshape(N_HI, N_LO, AMPS)
    return total
```

```python
import functools

import jax
import jax.numpy as jnp
from jax import lax
from jax.experimental import pallas as pl
from jax.experimental.pallas import tpu as pltpu
from jax.sharding import PartitionSpec as P

BITS = 8
GATE = 256
CLOSED = 2


def permuted(gate, order):
    rows = jnp.arange(GATE, dtype=jnp.int32)
    picked = rows[:, None] >> order[None, :] & 1
    weights = jnp.left_shift(jnp.ones((BITS,), jnp.int32), jnp.arange(BITS, dtype=jnp.int32))
    source = jnp.sum(picked * weights[None, :], axis=1)
    return jnp.take(gate, source, axis=0)


def local_plain(state_block, gate_table, closing_table, slice_edges, bit_orders):
    count_hi = lax.axis_size("hi")
    count_lo = lax.axis_size("lo")
    span_hi = GATE // count_hi
    span_lo = GATE // count_lo
    middle = state_block.shape[2] // (GATE * GATE * CLOSED)
    tensor = state_block.reshape(span_hi, count_hi, CLOSED, middle, count_lo, span_lo)
    turns = slice_edges.shape[0]
    firsts = []
    seconds = []
    fronts = []
    rears = []
    for turn_index in range(turns):
        chosen = slice_edges[turn_index]
        firsts.append(permuted(gate_table[chosen[0]], bit_orders[0]))
        seconds.append(permuted(gate_table[chosen[1]], bit_orders[1]))
        fronts.append(closing_table[chosen[2], 0])
        rears.append(closing_table[chosen[2], 1])
    section_ones = []
    for turn_index in range(turns):

        def apply_first(piece, first=firsts[turn_index], front=fronts[turn_index]):
            shape = piece.shape
            flat = piece.reshape(GATE, -1)
            product = lax.dot_general(
                first,
                flat,
                (((0,), (0,)), ((), ())),
                precision=lax.Precision.HIGHEST,
                preferred_element_type=jnp.float32,
            )
            scaled = jnp.transpose(front).reshape(shape[0], shape[1], shape[2], 1, 1, 1)
            return product.reshape(shape) * scaled

        section_ones.append(
            apply_first(lax.all_to_all(tensor, "hi", split_axis=1, concat_axis=1, tiled=True))
        )
    total = jnp.zeros((span_hi, count_hi, middle, count_lo, span_lo), jnp.float32)
    for turn_index in range(turns):
        current = section_ones[turn_index]

        def apply_second(piece, second=seconds[turn_index], rear=rears[turn_index]):
            shape = piece.shape
            flat = piece.reshape(-1, GATE)
            product = jnp.dot(
                flat, second, precision=lax.Precision.HIGHEST, preferred_element_type=jnp.float32
            )
            product = product.reshape(shape[0], shape[1], shape[2], shape[3], GATE)
            closed = jnp.einsum("phzkg,zg->phkg", product, rear, precision=lax.Precision.HIGHEST)
            return closed.reshape(shape[0], shape[1], shape[3], shape[4], shape[5])

        total = total + apply_second(
            lax.all_to_all(current, "lo", split_axis=4, concat_axis=4, tiled=True)
        )
    placed = lax.all_to_all(
        lax.all_to_all(total, "hi", split_axis=1, concat_axis=1, tiled=True),
        "lo",
        split_axis=3,
        concat_axis=3,
        tiled=True,
    )
    summed = lax.psum_scatter(placed.reshape(-1), "cuts", scatter_dimension=0, tiled=True)
    return summed.reshape(1, 1, -1)


MESH = pl.DeviceIdType.MESH
HALF = jnp.bfloat16
FULL = jnp.float32


def dot(left, right, dims=((1,), (0,))):
    return lax.dot_general(left, right, (dims, ((), ())), preferred_element_type=FULL)


def halves(value):
    high = value.astype(HALF)
    return high, (value - high.astype(FULL)).astype(HALF)


def source_row(index, orders_ref, section):
    total = jnp.zeros_like(index)
    for bit in range(BITS):
        picked = lax.shift_right_logical(index, jnp.full_like(index, orders_ref[section, bit])) & 1
        total = total | (picked << bit)
    return total


def kernel(
    count_hi,
    count_lo,
    x_hbm,
    gate_hbm,
    closing_hbm,
    edges_hbm,
    orders_hbm,
    out_ref,
    x_ref,
    gate_ref,
    closing_ref,
    edges_ref,
    orders_ref,
    outgoing,
    arrived,
    edges_far,
    first_ref,
    second_ref,
    part_near,
    part_far,
    result,
    landed,
    local_sems,
    edge_sems,
    part_sems,
    in_send,
    in_recv,
    out_send,
    out_recv,
):
    hi, lo, cut = lax.axis_index("hi"), lax.axis_index("lo"), lax.axis_index("cuts")
    other = 1 - cut
    span_hi, span_lo = GATE // count_hi, GATE // count_lo
    rows = GATE // 2
    turns = edges_ref.shape[0]
    edges = gate_ref.shape[0]
    offsets = [
        (a, b) for a in range(count_hi - 1, -1, -1) for b in range(count_lo) if a or b
    ]
    pairs = (
        (x_hbm, x_ref),
        (edges_hbm, edges_ref),
        (orders_hbm, orders_ref),
        (closing_hbm, closing_ref),
        (gate_hbm, gate_ref),
    )
    gets = [pltpu.make_async_copy(*pair, local_sems.at[i]) for i, pair in enumerate(pairs)]
    for get in gets:
        get.start()

    def target(a, b):
        return lax.rem(hi + a, count_hi), lax.rem(lo + b, count_lo)

    barrier = pltpu.get_barrier_semaphore()
    for a, b in offsets:
        th, tl = target(a, b)
        pl.semaphore_signal(barrier, inc=1, device_id={"hi": th, "lo": tl}, device_id_type=MESH)
    pl.semaphore_signal(barrier, inc=1, device_id={"cuts": other}, device_id_type=MESH)

    gets[0].wait()
    stride = count_hi * CLOSED * count_lo
    for b in range(count_hi):
        for e in range(count_lo):
            start = b * CLOSED * count_lo + cut * count_lo + e
            outgoing[b * count_lo + e] = x_ref[pl.ds(start, span_hi, stride=stride), :]
    arrived[lo, pl.ds(pl.multiple_of(hi * span_hi, span_hi), span_hi), :] = outgoing[
        hi * count_lo + lo
    ]
    pl.semaphore_wait(barrier, len(offsets) + 1)

    sends = []
    for k, (a, b) in enumerate(offsets):
        th, tl = target(a, b)
        copy = pltpu.make_async_remote_copy(
            src_ref=outgoing.at[th * count_lo + tl],
            dst_ref=arrived.at[lo, pl.ds(pl.multiple_of(hi * span_hi, span_hi), span_hi), :],
            send_sem=in_send.at[k],
            recv_sem=in_recv.at[k],
            device_id={"hi": th, "lo": tl},
            device_id_type=MESH,
        )
        copy.start()
        sends.append(copy)
    gets[1].wait()
    edge_copy = pltpu.make_async_remote_copy(
        src_ref=edges_ref,
        dst_ref=edges_far,
        send_sem=edge_sems.at[0],
        recv_sem=edge_sems.at[1],
        device_id={"cuts": other},
        device_id_type=MESH,
    )
    edge_copy.start()

    gets[2].wait()
    down = lax.broadcasted_iota(jnp.int32, (GATE, GATE), 0)
    along = lax.broadcasted_iota(jnp.int32, (GATE, GATE), 1)
    per = span_hi // 2
    column = (down // rows * per + down % per) * count_hi + down % rows // per
    columns = (column == along).astype(FULL).astype(HALF)
    rows_one = source_row(along % span_hi * count_hi + along // span_hi, orders_ref, 0)
    rows_one = (rows_one == down).astype(FULL).astype(HALF)
    rows_two = (source_row(down, orders_ref, 1) == along).astype(FULL).astype(HALF)

    gets[3].wait()
    gets[4].wait()
    edge_copy.wait()
    for s in range(2 * turns):
        chosen = edges_ref if s < turns else edges_far
        turn = s % turns

        def pick(place, values):
            total = None
            for c in range(edges):
                weight = (chosen[turn : turn + 1, place : place + 1] == c).astype(FULL)
                term = weight * values(c)
                total = term if total is None else total + term
            return total

        front = pick(2, lambda c: closing_ref[c, 0, pl.ds(cut, 1), :])
        rear = pick(2, lambda c: closing_ref[c, 1, pl.ds(cut, 1), :])
        for part, piece in enumerate(halves(pick(0, lambda c: gate_ref[c]) * front)):
            moved = dot(columns, piece, ((1,), (1,))).astype(HALF)
            moved = dot(moved, rows_one).astype(HALF)
            for side in range(2):
                first_ref[part, side, pl.ds(s * rows, rows), :] = moved[
                    side * rows : (side + 1) * rows
                ]
        for part, piece in enumerate(halves(pick(1, lambda c: gate_ref[c]) * rear)):
            second_ref[part, pl.ds(s * GATE, GATE), :] = dot(rows_two, piece).astype(HALF)

    for copy in sends:
        copy.wait_recv()
    x_high, x_low = halves(jnp.concatenate([arrived[i] for i in range(count_lo)], axis=1))

    def amplitudes(side):
        high, low = first_ref[0, side], first_ref[1, side]
        inner = dot(high, x_high) + dot(high, x_low) + dot(low, x_high)
        inner_high, inner_low = halves(inner)
        total = None
        for s in range(2 * turns):
            left_high = inner_high[s * rows : (s + 1) * rows]
            left_low = inner_low[s * rows : (s + 1) * rows]
            right_high = second_ref[0, pl.ds(s * GATE, GATE), :]
            right_low = second_ref[1, pl.ds(s * GATE, GATE), :]
            term = dot(left_high, right_high) + dot(left_high, right_low) + dot(left_low, right_high)
            total = term if total is None else total + term
        return total

    part_near[...] = amplitudes(other)
    part_copy = pltpu.make_async_remote_copy(
        src_ref=part_near,
        dst_ref=part_far,
        send_sem=part_sems.at[0],
        recv_sem=part_sems.at[1],
        device_id={"cuts": other},
        device_id_type=MESH,
    )
    part_copy.start()
    own = amplitudes(cut)
    part_copy.wait_recv()
    own = own + part_far[...]
    for b in range(count_hi):
        for e in range(count_lo):
            result[b * count_lo + e] = own[b * per : (b + 1) * per, e * span_lo : (e + 1) * span_lo]
    here = hi * count_lo + lo
    outs = []
    for k, (a, b) in enumerate(offsets):
        th, tl = target(a, b)
        copy = pltpu.make_async_remote_copy(
            src_ref=result.at[th * count_lo + tl],
            dst_ref=landed.at[here],
            send_sem=out_send.at[k],
            recv_sem=out_recv.at[k],
            device_id={"hi": th, "lo": tl},
            device_id_type=MESH,
        )
        copy.start()
        outs.append(copy)
    landed[here] = result[here]
    for copy in outs:
        copy.wait_recv()
    for j in range(count_hi * count_lo):
        out_ref[pl.ds(j, per, stride=count_hi * count_lo), :] = landed[j]
    for copy in sends:
        copy.wait_send()
    part_copy.wait_send()
    for copy in outs:
        copy.wait_send()


def local(state_block, gate_table, closing_table, slice_edges, bit_orders):
    count_hi = lax.axis_size("hi")
    count_lo = lax.axis_size("lo")
    span_hi = GATE // count_hi
    span_lo = GATE // count_lo
    blocks = count_hi * count_lo
    middle = state_block.shape[2] // (GATE * GATE * CLOSED)
    fits = middle == 1 and span_lo == 128 and span_hi % 16 == 0
    if not fits or lax.axis_size("cuts") != CLOSED:
        return local_plain(state_block, gate_table, closing_table, slice_edges, bit_orders)
    slices = slice_edges.shape[0] * CLOSED
    rows = GATE // 2
    hbm = pl.BlockSpec(memory_space=pltpu.HBM)
    dma = pltpu.SemaphoreType.DMA
    out = pl.pallas_call(
        functools.partial(kernel, count_hi, count_lo),
        out_shape=jax.ShapeDtypeStruct((span_hi // 2 * blocks, span_lo), FULL),
        in_specs=[hbm] * 5,
        out_specs=pl.BlockSpec(memory_space=pltpu.VMEM),
        scratch_shapes=[
            pltpu.VMEM((span_hi * blocks * CLOSED, span_lo), FULL),
            pltpu.VMEM(gate_table.shape, FULL),
            pltpu.VMEM(closing_table.shape, FULL),
            pltpu.VMEM(slice_edges.shape, jnp.int32),
            pltpu.SMEM(bit_orders.shape, jnp.int32),
            pltpu.VMEM((blocks, span_hi, span_lo), FULL),
            pltpu.VMEM((count_lo, GATE, span_lo), FULL),
            pltpu.VMEM(slice_edges.shape, jnp.int32),
            pltpu.VMEM((2, 2, slices * rows, GATE), HALF),
            pltpu.VMEM((2, slices * GATE, GATE), HALF),
            pltpu.VMEM((rows, GATE), FULL),
            pltpu.VMEM((rows, GATE), FULL),
            pltpu.VMEM((blocks, span_hi // 2, span_lo), FULL),
            pltpu.VMEM((blocks, span_hi // 2, span_lo), FULL),
            dma((5,)),
            dma((2,)),
            dma((2,)),
            dma((blocks,)),
            dma((blocks,)),
            dma((blocks,)),
            dma((blocks,)),
        ],
        compiler_params=pltpu.CompilerParams(
            collective_id=0, has_side_effects=True, vmem_limit_bytes=32 * 1024 * 1024
        ),
    )(
        state_block.reshape(-1, span_lo),
        gate_table,
        closing_table,
        slice_edges,
        bit_orders,
    )
    return out.reshape(1, 1, -1)


def solution(mesh):
    in_specs = (P(("group", "hi"), "lo", None), P(), P(), P(("group", "cuts"), None), P())
    out_specs = P(("group", "hi"), "lo", "cuts")
    return jax.shard_map(local, mesh=mesh, in_specs=in_specs, out_specs=out_specs, check_vma=False)
```

```python
import functools

import jax
import jax.numpy as jnp
from jax import lax
from jax.experimental import pallas as pl
from jax.experimental.pallas import tpu as pltpu
from jax.sharding import PartitionSpec as P

BITS = 8
GATE = 256
CLOSED = 2


def permuted(gate, order):
    rows = jnp.arange(GATE, dtype=jnp.int32)
    picked = rows[:, None] >> order[None, :] & 1
    weights = jnp.left_shift(jnp.ones((BITS,), jnp.int32), jnp.arange(BITS, dtype=jnp.int32))
    source = jnp.sum(picked * weights[None, :], axis=1)
    return jnp.take(gate, source, axis=0)


def local_plain(state_block, gate_table, closing_table, slice_edges, bit_orders):
    count_hi = lax.axis_size("hi")
    count_lo = lax.axis_size("lo")
    span_hi = GATE // count_hi
    span_lo = GATE // count_lo
    middle = state_block.shape[2] // (GATE * GATE * CLOSED)
    tensor = state_block.reshape(span_hi, count_hi, CLOSED, middle, count_lo, span_lo)
    turns = slice_edges.shape[0]
    firsts = []
    seconds = []
    fronts = []
    rears = []
    for turn_index in range(turns):
        chosen = slice_edges[turn_index]
        firsts.append(permuted(gate_table[chosen[0]], bit_orders[0]))
        seconds.append(permuted(gate_table[chosen[1]], bit_orders[1]))
        fronts.append(closing_table[chosen[2], 0])
        rears.append(closing_table[chosen[2], 1])
    section_ones = []
    for turn_index in range(turns):

        def apply_first(piece, first=firsts[turn_index], front=fronts[turn_index]):
            shape = piece.shape
            flat = piece.reshape(GATE, -1)
            product = lax.dot_general(
                first,
                flat,
                (((0,), (0,)), ((), ())),
                precision=lax.Precision.HIGHEST,
                preferred_element_type=jnp.float32,
            )
            scaled = jnp.transpose(front).reshape(shape[0], shape[1], shape[2], 1, 1, 1)
            return product.reshape(shape) * scaled

        section_ones.append(
            apply_first(lax.all_to_all(tensor, "hi", split_axis=1, concat_axis=1, tiled=True))
        )
    total = jnp.zeros((span_hi, count_hi, middle, count_lo, span_lo), jnp.float32)
    for turn_index in range(turns):
        current = section_ones[turn_index]

        def apply_second(piece, second=seconds[turn_index], rear=rears[turn_index]):
            shape = piece.shape
            flat = piece.reshape(-1, GATE)
            product = jnp.dot(
                flat, second, precision=lax.Precision.HIGHEST, preferred_element_type=jnp.float32
            )
            product = product.reshape(shape[0], shape[1], shape[2], shape[3], GATE)
            closed = jnp.einsum("phzkg,zg->phkg", product, rear, precision=lax.Precision.HIGHEST)
            return closed.reshape(shape[0], shape[1], shape[3], shape[4], shape[5])

        total = total + apply_second(
            lax.all_to_all(current, "lo", split_axis=4, concat_axis=4, tiled=True)
        )
    placed = lax.all_to_all(
        lax.all_to_all(total, "hi", split_axis=1, concat_axis=1, tiled=True),
        "lo",
        split_axis=3,
        concat_axis=3,
        tiled=True,
    )
    summed = lax.psum_scatter(placed.reshape(-1), "cuts", scatter_dimension=0, tiled=True)
    return summed.reshape(1, 1, -1)


MESH = pl.DeviceIdType.MESH
HALF = jnp.bfloat16
FULL = jnp.float32


def dot(left, right, dims=((1,), (0,))):
    return lax.dot_general(left, right, (dims, ((), ())), preferred_element_type=FULL)


def halves(value):
    high = value.astype(HALF)
    return high, (value - high.astype(FULL)).astype(HALF)


def source_row(index, orders_ref, section):
    total = jnp.zeros_like(index)
    for bit in range(BITS):
        picked = lax.shift_right_logical(index, jnp.full_like(index, orders_ref[section, bit])) & 1
        total = total | (picked << bit)
    return total


def flipped(index, mask):
    bit = 1
    while bit <= mask:
        if mask & bit:
            index = index + bit - 2 * bit * (index // bit % 2)
        bit *= 2
    return index


def kernel(
    group,
    order,
    count_hi,
    count_lo,
    x_hbm,
    gate_hbm,
    closing_hbm,
    edges_hbm,
    orders_hbm,
    out_ref,
    x_ref,
    gate_ref,
    closing_ref,
    edges_ref,
    orders_ref,
    outgoing,
    arrived,
    edges_far,
    first_ref,
    second_ref,
    sums,
    part_near,
    part_far,
    result,
    landed,
    local_sems,
    edge_sems,
    part_sems,
    in_send,
    in_recv,
    out_send,
    out_recv,
):
    hi, lo, cut = lax.axis_index("hi"), lax.axis_index("lo"), lax.axis_index("cuts")
    other = 1 - cut
    span_hi, span_lo = GATE // count_hi, GATE // count_lo
    rows = GATE // 2
    turns = edges_ref.shape[0]
    edges = gate_ref.shape[0]
    offsets = [
        (a, b) for a in range(count_hi) for b in range(count_lo) if a or b
    ]
    pairs = (
        (x_hbm, x_ref),
        (edges_hbm, edges_ref),
        (orders_hbm, orders_ref),
        (closing_hbm, closing_ref),
        (gate_hbm, gate_ref),
    )
    gets = [pltpu.make_async_copy(*pair, local_sems.at[i]) for i, pair in enumerate(pairs)]
    for get in gets:
        get.start()

    def target(a, b):
        return flipped(hi, a), flipped(lo, b)

    barrier = pltpu.get_barrier_semaphore()
    for a, b in offsets:
        th, tl = target(a, b)
        pl.semaphore_signal(barrier, inc=1, device_id={"hi": th, "lo": tl}, device_id_type=MESH)
    pl.semaphore_signal(barrier, inc=1, device_id={"cuts": other}, device_id_type=MESH)

    gets[0].wait()
    stride = count_hi * CLOSED * count_lo
    for b in range(count_hi):
        for e in range(count_lo):
            start = b * CLOSED * count_lo + cut * count_lo + e
            outgoing[b * count_lo + e] = x_ref[pl.ds(start, span_hi, stride=stride), :]
    arrived[lo, pl.ds(pl.multiple_of(hi * span_hi, span_hi), span_hi), :] = outgoing[
        hi * count_lo + lo
    ]
    pl.semaphore_wait(barrier, len(offsets) + 1)

    sends = []
    for k, (a, b) in enumerate(offsets):
        th, tl = target(a, b)
        copy = pltpu.make_async_remote_copy(
            src_ref=outgoing.at[th * count_lo + tl],
            dst_ref=arrived.at[lo, pl.ds(pl.multiple_of(hi * span_hi, span_hi), span_hi), :],
            send_sem=in_send.at[k],
            recv_sem=in_recv.at[k],
            device_id={"hi": th, "lo": tl},
            device_id_type=MESH,
        )
        sends.append(copy)
    for k in [0] + list(range(len(offsets) - 1, 0, -1)):
        sends[k].start()
    gets[1].wait()
    edge_copy = pltpu.make_async_remote_copy(
        src_ref=edges_ref,
        dst_ref=edges_far,
        send_sem=edge_sems.at[0],
        recv_sem=edge_sems.at[1],
        device_id={"cuts": other},
        device_id_type=MESH,
    )
    edge_copy.start()

    gets[2].wait()
    down = lax.broadcasted_iota(jnp.int32, (GATE, GATE), 0)
    along = lax.broadcasted_iota(jnp.int32, (GATE, GATE), 1)
    per = span_hi // 2
    wide = group * span_hi
    column = (down // rows * per + down % per) * count_hi + down % rows // per
    columns = (column == along).astype(FULL).astype(HALF)
    rows_one = source_row(along % span_hi * count_hi + along // span_hi, orders_ref, 0)
    rows_one = (rows_one == down).astype(FULL).astype(HALF)
    rows_two = (source_row(down, orders_ref, 1) == along).astype(FULL).astype(HALF)

    gets[3].wait()
    gets[4].wait()
    edge_copy.wait()
    for s in range(2 * turns):
        chosen = edges_ref if s < turns else edges_far
        turn = s % turns

        def pick(place, values):
            total = None
            for c in range(edges):
                weight = (chosen[turn : turn + 1, place : place + 1] == c).astype(FULL)
                term = weight * values(c)
                total = term if total is None else total + term
            return total

        front = pick(2, lambda c: closing_ref[c, 0, pl.ds(cut, 1), :])
        rear = pick(2, lambda c: closing_ref[c, 1, pl.ds(cut, 1), :])
        for part, piece in enumerate(halves(pick(0, lambda c: gate_ref[c]) * front)):
            moved = dot(columns, piece, ((1,), (1,))).astype(HALF)
            moved = dot(moved, rows_one).astype(HALF)
            for side in range(2):
                for c in range(count_hi // group):
                    first_ref[part, c, side, :, s * wide : (s + 1) * wide] = moved[
                        side * rows : (side + 1) * rows, c * wide : (c + 1) * wide
                    ]
        for part, piece in enumerate(halves(pick(1, lambda c: gate_ref[c]) * rear)):
            second_ref[part, s] = dot(rows_two, piece).astype(HALF)

    def advance(step):
        for copy, (a, b) in zip(sends, offsets):
            if a // group == step:
                copy.wait_recv()
        c = flipped(hi // group, step)
        place = pl.ds(pl.multiple_of(c * wide, wide), wide)
        piece = jnp.concatenate([arrived[i, place, :] for i in range(count_lo)], axis=1)
        high, low = halves(piece)
        inner = []
        for s in range(2 * turns):
            inner.append(
                dot(high, second_ref[0, s]) + dot(low, second_ref[0, s]) + dot(high, second_ref[1, s])
            )
        high, low = halves(jnp.concatenate(inner, axis=0))

        def side_sum(side):
            left, rest = first_ref[0, c, side], first_ref[1, c, side]
            return dot(left, high) + dot(left, low) + dot(rest, high)

        return side_sum

    for i, step in enumerate(order[:-1]):
        side_sum = advance(step)
        for side in range(2):
            if i == 0:
                sums[side] = side_sum(side)
            else:
                sums[side] += side_sum(side)
    side_sum = advance(order[-1])
    part_near[...] = sums[other] + side_sum(other)
    part_copy = pltpu.make_async_remote_copy(
        src_ref=part_near,
        dst_ref=part_far,
        send_sem=part_sems.at[0],
        recv_sem=part_sems.at[1],
        device_id={"cuts": other},
        device_id_type=MESH,
    )
    part_copy.start()
    own = sums[cut] + side_sum(cut)
    part_copy.wait_recv()
    own = own + part_far[...]
    for b in range(count_hi):
        for e in range(count_lo):
            result[b * count_lo + e] = own[b * per : (b + 1) * per, e * span_lo : (e + 1) * span_lo]
    here = hi * count_lo + lo
    outs = []
    for k, (a, b) in enumerate(offsets):
        th, tl = target(a, b)
        copy = pltpu.make_async_remote_copy(
            src_ref=result.at[th * count_lo + tl],
            dst_ref=landed.at[here],
            send_sem=out_send.at[k],
            recv_sem=out_recv.at[k],
            device_id={"hi": th, "lo": tl},
            device_id_type=MESH,
        )
        copy.start()
        outs.append(copy)
    landed[here] = result[here]
    for copy in outs:
        copy.wait_recv()
    for j in range(count_hi * count_lo):
        out_ref[pl.ds(j, per, stride=count_hi * count_lo), :] = landed[j]
    for copy in sends:
        copy.wait_send()
    part_copy.wait_send()
    for copy in outs:
        copy.wait_send()


def local(state_block, gate_table, closing_table, slice_edges, bit_orders):
    count_hi = lax.axis_size("hi")
    count_lo = lax.axis_size("lo")
    span_hi = GATE // count_hi
    span_lo = GATE // count_lo
    blocks = count_hi * count_lo
    middle = state_block.shape[2] // (GATE * GATE * CLOSED)
    fits = middle == 1 and span_lo == 128 and span_hi % 16 == 0
    if not fits or lax.axis_size("cuts") != CLOSED:
        return local_plain(state_block, gate_table, closing_table, slice_edges, bit_orders)
    group = 1
    order = (0, 1, 3, 2) if count_hi == 4 else tuple(range(count_hi // group))
    slices = slice_edges.shape[0] * CLOSED
    rows = GATE // 2
    hbm = pl.BlockSpec(memory_space=pltpu.HBM)
    dma = pltpu.SemaphoreType.DMA
    out = pl.pallas_call(
        functools.partial(kernel, group, order, count_hi, count_lo),
        out_shape=jax.ShapeDtypeStruct((span_hi // 2 * blocks, span_lo), FULL),
        in_specs=[hbm] * 5,
        out_specs=pl.BlockSpec(memory_space=pltpu.VMEM),
        scratch_shapes=[
            pltpu.VMEM((span_hi * blocks * CLOSED, span_lo), FULL),
            pltpu.VMEM(gate_table.shape, FULL),
            pltpu.VMEM(closing_table.shape, FULL),
            pltpu.VMEM(slice_edges.shape, jnp.int32),
            pltpu.SMEM(bit_orders.shape, jnp.int32),
            pltpu.VMEM((blocks, span_hi, span_lo), FULL),
            pltpu.VMEM((count_lo, GATE, span_lo), FULL),
            pltpu.VMEM(slice_edges.shape, jnp.int32),
            pltpu.VMEM((2, count_hi // group, 2, rows, slices * group * span_hi), HALF),
            pltpu.VMEM((2, slices, GATE, GATE), HALF),
            pltpu.VMEM((2, rows, GATE), FULL),
            pltpu.VMEM((rows, GATE), FULL),
            pltpu.VMEM((rows, GATE), FULL),
            pltpu.VMEM((blocks, span_hi // 2, span_lo), FULL),
            pltpu.VMEM((blocks, span_hi // 2, span_lo), FULL),
            dma((5,)),
            dma((2,)),
            dma((2,)),
            dma((blocks,)),
            dma((blocks,)),
            dma((blocks,)),
            dma((blocks,)),
        ],
        compiler_params=pltpu.CompilerParams(
            collective_id=0, has_side_effects=True, vmem_limit_bytes=67_043_328
        ),
    )(
        state_block.reshape(-1, span_lo),
        gate_table,
        closing_table,
        slice_edges,
        bit_orders,
    )
    return out.reshape(1, 1, -1)


def solution(mesh):
    in_specs = (P(("group", "hi"), "lo", None), P(), P(), P(("group", "cuts"), None), P())
    out_specs = P(("group", "hi"), "lo", "cuts")
    return jax.shard_map(local, mesh=mesh, in_specs=in_specs, out_specs=out_specs, check_vma=False)
```

```python
import functools

import jax
import jax.numpy as jnp
from jax import lax
from jax.experimental import pallas as pl
from jax.experimental.pallas import tpu as pltpu
from jax.sharding import PartitionSpec as P

BITS = 8
GATE = 256
CLOSED = 2


def permuted(gate, order):
    rows = jnp.arange(GATE, dtype=jnp.int32)
    picked = rows[:, None] >> order[None, :] & 1
    weights = jnp.left_shift(jnp.ones((BITS,), jnp.int32), jnp.arange(BITS, dtype=jnp.int32))
    source = jnp.sum(picked * weights[None, :], axis=1)
    return jnp.take(gate, source, axis=0)


def local_plain(state_block, gate_table, closing_table, slice_edges, bit_orders):
    count_hi = lax.axis_size("hi")
    count_lo = lax.axis_size("lo")
    span_hi = GATE // count_hi
    span_lo = GATE // count_lo
    middle = state_block.shape[2] // (GATE * GATE * CLOSED)
    tensor = state_block.reshape(span_hi, count_hi, CLOSED, middle, count_lo, span_lo)
    turns = slice_edges.shape[0]
    firsts = []
    seconds = []
    fronts = []
    rears = []
    for turn_index in range(turns):
        chosen = slice_edges[turn_index]
        firsts.append(permuted(gate_table[chosen[0]], bit_orders[0]))
        seconds.append(permuted(gate_table[chosen[1]], bit_orders[1]))
        fronts.append(closing_table[chosen[2], 0])
        rears.append(closing_table[chosen[2], 1])
    section_ones = []
    for turn_index in range(turns):

        def apply_first(piece, first=firsts[turn_index], front=fronts[turn_index]):
            shape = piece.shape
            flat = piece.reshape(GATE, -1)
            product = lax.dot_general(
                first,
                flat,
                (((0,), (0,)), ((), ())),
                precision=lax.Precision.HIGHEST,
                preferred_element_type=jnp.float32,
            )
            scaled = jnp.transpose(front).reshape(shape[0], shape[1], shape[2], 1, 1, 1)
            return product.reshape(shape) * scaled

        section_ones.append(
            apply_first(lax.all_to_all(tensor, "hi", split_axis=1, concat_axis=1, tiled=True))
        )
    total = jnp.zeros((span_hi, count_hi, middle, count_lo, span_lo), jnp.float32)
    for turn_index in range(turns):
        current = section_ones[turn_index]

        def apply_second(piece, second=seconds[turn_index], rear=rears[turn_index]):
            shape = piece.shape
            flat = piece.reshape(-1, GATE)
            product = jnp.dot(
                flat, second, precision=lax.Precision.HIGHEST, preferred_element_type=jnp.float32
            )
            product = product.reshape(shape[0], shape[1], shape[2], shape[3], GATE)
            closed = jnp.einsum("phzkg,zg->phkg", product, rear, precision=lax.Precision.HIGHEST)
            return closed.reshape(shape[0], shape[1], shape[3], shape[4], shape[5])

        total = total + apply_second(
            lax.all_to_all(current, "lo", split_axis=4, concat_axis=4, tiled=True)
        )
    placed = lax.all_to_all(
        lax.all_to_all(total, "hi", split_axis=1, concat_axis=1, tiled=True),
        "lo",
        split_axis=3,
        concat_axis=3,
        tiled=True,
    )
    summed = lax.psum_scatter(placed.reshape(-1), "cuts", scatter_dimension=0, tiled=True)
    return summed.reshape(1, 1, -1)


MESH = pl.DeviceIdType.MESH
HALF = jnp.bfloat16
FULL = jnp.float32


def dot(left, right, dims=((1,), (0,))):
    return lax.dot_general(left, right, (dims, ((), ())), preferred_element_type=FULL)


def halves(value):
    high = value.astype(HALF)
    return high, (value - high.astype(FULL)).astype(HALF)


def source_row(index, orders_ref, section):
    total = jnp.zeros_like(index)
    for bit in range(BITS):
        picked = lax.shift_right_logical(index, jnp.full_like(index, orders_ref[section, bit])) & 1
        total = total | (picked << bit)
    return total


def flipped(index, mask):
    bit = 1
    while bit <= mask:
        if mask & bit:
            index = index + bit - 2 * bit * (index // bit % 2)
        bit *= 2
    return index


def kernel(
    group,
    order,
    count_hi,
    count_lo,
    x_hbm,
    gate_hbm,
    closing_hbm,
    edges_hbm,
    orders_hbm,
    out_ref,
    x_ref,
    gate_ref,
    closing_ref,
    edges_ref,
    orders_ref,
    outgoing,
    arrived,
    edges_far,
    first_ref,
    second_ref,
    sums,
    part_near,
    part_far,
    result,
    landed,
    local_sems,
    edge_sems,
    part_sems,
    in_send,
    in_recv,
    out_send,
    out_recv,
):
    hi, lo, cut = lax.axis_index("hi"), lax.axis_index("lo"), lax.axis_index("cuts")
    other = 1 - cut
    span_hi, span_lo = GATE // count_hi, GATE // count_lo
    rows = GATE // 2
    turns = edges_ref.shape[0]
    edges = gate_ref.shape[0]
    offsets = [
        (a, b) for a in range(count_hi) for b in range(count_lo) if a or b
    ]
    pairs = (
        (x_hbm, x_ref),
        (edges_hbm, edges_ref),
        (orders_hbm, orders_ref),
        (closing_hbm, closing_ref),
        (gate_hbm, gate_ref),
    )
    gets = [pltpu.make_async_copy(*pair, local_sems.at[i]) for i, pair in enumerate(pairs)]
    for get in gets:
        get.start()

    def target(a, b):
        return flipped(hi, a), flipped(lo, b)

    barrier = pltpu.get_barrier_semaphore()
    for a, b in offsets:
        th, tl = target(a, b)
        pl.semaphore_signal(barrier, inc=1, device_id={"hi": th, "lo": tl}, device_id_type=MESH)
    pl.semaphore_signal(barrier, inc=1, device_id={"cuts": other}, device_id_type=MESH)

    gets[0].wait()
    stride = count_hi * CLOSED * count_lo
    for b in range(count_hi):
        for e in range(count_lo):
            start = b * CLOSED * count_lo + cut * count_lo + e
            outgoing[b * count_lo + e] = x_ref[pl.ds(start, span_hi, stride=stride), :]
    arrived[lo, pl.ds(pl.multiple_of(hi * span_hi, span_hi), span_hi), :] = outgoing[
        hi * count_lo + lo
    ]
    pl.semaphore_wait(barrier, len(offsets) + 1)

    sends = []
    for k, (a, b) in enumerate(offsets):
        th, tl = target(a, b)
        copy = pltpu.make_async_remote_copy(
            src_ref=outgoing.at[th * count_lo + tl],
            dst_ref=arrived.at[lo, pl.ds(pl.multiple_of(hi * span_hi, span_hi), span_hi), :],
            send_sem=in_send.at[k],
            recv_sem=in_recv.at[k],
            device_id={"hi": th, "lo": tl},
            device_id_type=MESH,
        )
        sends.append(copy)
    for k in [0] + list(range(len(offsets) - 1, 0, -1)):
        sends[k].start()
    gets[1].wait()
    edge_copy = pltpu.make_async_remote_copy(
        src_ref=edges_ref,
        dst_ref=edges_far,
        send_sem=edge_sems.at[0],
        recv_sem=edge_sems.at[1],
        device_id={"cuts": other},
        device_id_type=MESH,
    )
    edge_copy.start()

    gets[2].wait()
    down = lax.broadcasted_iota(jnp.int32, (GATE, GATE), 0)
    along = lax.broadcasted_iota(jnp.int32, (GATE, GATE), 1)
    per = span_hi // 2
    wide = group * span_hi
    column = (down // rows * per + down % per) * count_hi + down % rows // per
    columns = (column == along).astype(FULL).astype(HALF)
    rows_one = source_row(along % span_hi * count_hi + along // span_hi, orders_ref, 0)
    rows_one = (rows_one == down).astype(FULL).astype(HALF)
    rows_two = (source_row(down, orders_ref, 1) == along).astype(FULL).astype(HALF)

    gets[3].wait()
    gets[4].wait()
    edge_copy.wait()
    for s in range(2 * turns):
        chosen = edges_ref if s < turns else edges_far
        turn = s % turns

        def pick(place, values):
            total = None
            for c in range(edges):
                weight = (chosen[turn : turn + 1, place : place + 1] == c).astype(FULL)
                term = weight * values(c)
                total = term if total is None else total + term
            return total

        front = pick(2, lambda c: closing_ref[c, 0, pl.ds(cut, 1), :])
        rear = pick(2, lambda c: closing_ref[c, 1, pl.ds(cut, 1), :])
        for part, piece in enumerate(halves(pick(0, lambda c: gate_ref[c]) * front)):
            moved = dot(columns, piece, ((1,), (1,))).astype(HALF)
            moved = dot(moved, rows_one).astype(HALF)
            for side in range(2):
                for c in range(count_hi // group):
                    first_ref[part, c, side, :, s * wide : (s + 1) * wide] = moved[
                        side * rows : (side + 1) * rows, c * wide : (c + 1) * wide
                    ]
        for part, piece in enumerate(halves(pick(1, lambda c: gate_ref[c]) * rear)):
            second_ref[part, s] = dot(rows_two, piece).astype(HALF)

    def advance(step):
        for copy, (a, b) in zip(sends, offsets):
            if a // group == step:
                copy.wait_recv()
        c = flipped(hi // group, step)
        place = pl.ds(pl.multiple_of(c * wide, wide), wide)
        piece = jnp.concatenate([arrived[i, place, :] for i in range(count_lo)], axis=1)
        high, low = halves(piece)
        inner = []
        for s in range(2 * turns):
            inner.append(
                dot(high, second_ref[0, s]) + dot(low, second_ref[0, s]) + dot(high, second_ref[1, s])
            )
        high, low = halves(jnp.concatenate(inner, axis=0))

        def side_sum(side):
            left, rest = first_ref[0, c, side], first_ref[1, c, side]
            return dot(left, high) + dot(left, low) + dot(rest, high)

        return side_sum

    for i, step in enumerate(order[:-1]):
        side_sum = advance(step)
        for side in range(2):
            if i == 0:
                sums[side] = side_sum(side)
            else:
                sums[side] += side_sum(side)
    side_sum = advance(order[-1])
    part_near[...] = sums[other] + side_sum(other)
    part_copy = pltpu.make_async_remote_copy(
        src_ref=part_near,
        dst_ref=part_far,
        send_sem=part_sems.at[0],
        recv_sem=part_sems.at[1],
        device_id={"cuts": other},
        device_id_type=MESH,
    )
    part_copy.start()
    own = sums[cut] + side_sum(cut)
    part_copy.wait_recv()
    own = own + part_far[...]
    for b in range(count_hi):
        for e in range(count_lo):
            result[b * count_lo + e] = own[b * per : (b + 1) * per, e * span_lo : (e + 1) * span_lo]
    here = hi * count_lo + lo
    outs = []
    for k, (a, b) in enumerate(offsets):
        th, tl = target(a, b)
        copy = pltpu.make_async_remote_copy(
            src_ref=result.at[th * count_lo + tl],
            dst_ref=landed.at[here],
            send_sem=out_send.at[k],
            recv_sem=out_recv.at[k],
            device_id={"hi": th, "lo": tl},
            device_id_type=MESH,
        )
        outs.append(copy)
    for k in range(len(offsets) - 1, -1, -1):
        outs[k].start()
    blocks = count_hi * count_lo
    out_ref[pl.ds(here, per, stride=blocks), :] = result[here]
    for copy, (a, b) in zip(outs, offsets):
        copy.wait_recv()
        th, tl = target(a, b)
        j = th * count_lo + tl
        out_ref[pl.ds(j, per, stride=blocks), :] = landed[j]
    for copy in sends:
        copy.wait_send()
    part_copy.wait_send()
    for copy in outs:
        copy.wait_send()


def local(state_block, gate_table, closing_table, slice_edges, bit_orders):
    count_hi = lax.axis_size("hi")
    count_lo = lax.axis_size("lo")
    span_hi = GATE // count_hi
    span_lo = GATE // count_lo
    blocks = count_hi * count_lo
    middle = state_block.shape[2] // (GATE * GATE * CLOSED)
    fits = middle == 1 and span_lo == 128 and span_hi % 16 == 0
    if not fits or lax.axis_size("cuts") != CLOSED:
        return local_plain(state_block, gate_table, closing_table, slice_edges, bit_orders)
    group = 1
    order = (0, 1, 3, 2) if count_hi == 4 else tuple(range(count_hi // group))
    slices = slice_edges.shape[0] * CLOSED
    rows = GATE // 2
    hbm = pl.BlockSpec(memory_space=pltpu.HBM)
    dma = pltpu.SemaphoreType.DMA
    out = pl.pallas_call(
        functools.partial(kernel, group, order, count_hi, count_lo),
        out_shape=jax.ShapeDtypeStruct((span_hi // 2 * blocks, span_lo), FULL),
        in_specs=[hbm] * 5,
        out_specs=pl.BlockSpec(memory_space=pltpu.VMEM),
        scratch_shapes=[
            pltpu.VMEM((span_hi * blocks * CLOSED, span_lo), FULL),
            pltpu.VMEM(gate_table.shape, FULL),
            pltpu.VMEM(closing_table.shape, FULL),
            pltpu.VMEM(slice_edges.shape, jnp.int32),
            pltpu.SMEM(bit_orders.shape, jnp.int32),
            pltpu.VMEM((blocks, span_hi, span_lo), FULL),
            pltpu.VMEM((count_lo, GATE, span_lo), FULL),
            pltpu.VMEM(slice_edges.shape, jnp.int32),
            pltpu.VMEM((2, count_hi // group, 2, rows, slices * group * span_hi), HALF),
            pltpu.VMEM((2, slices, GATE, GATE), HALF),
            pltpu.VMEM((2, rows, GATE), FULL),
            pltpu.VMEM((rows, GATE), FULL),
            pltpu.VMEM((rows, GATE), FULL),
            pltpu.VMEM((blocks, span_hi // 2, span_lo), FULL),
            pltpu.VMEM((blocks, span_hi // 2, span_lo), FULL),
            dma((5,)),
            dma((2,)),
            dma((2,)),
            dma((blocks,)),
            dma((blocks,)),
            dma((blocks,)),
            dma((blocks,)),
        ],
        compiler_params=pltpu.CompilerParams(
            collective_id=0, has_side_effects=True, vmem_limit_bytes=32 * 1024 * 1024
        ),
    )(
        *(
            pltpu.with_memory_space_constraint(item, pltpu.HBM)
            for item in (
                state_block.reshape(-1, span_lo),
                gate_table,
                closing_table,
                slice_edges,
                bit_orders,
            )
        )
    )
    return out.reshape(1, 1, -1)


def solution(mesh):
    in_specs = (P(("group", "hi"), "lo", None), P(), P(), P(("group", "cuts"), None), P())
    out_specs = P(("group", "hi"), "lo", "cuts")
    return jax.shard_map(local, mesh=mesh, in_specs=in_specs, out_specs=out_specs, check_vma=False)
```
